32 devices in a mesh: gx: 8 (over z, core), gy: 4 (over y, x).
Axes of the slice: x: 2, y: 2, z: 4, core: 2. Of those that a mesh axis runs over, the one named last changes fastest.
Arguments:
- tokens: bfloat16 [512, 4096], P('gx', 'gy'), may hold values from -6 to 6
- gate_blocks: bfloat16 [4, 8, 84, 128, 128], P('gy', 'gx'), may hold values from -0.125 to 0.125
- up_blocks: bfloat16 [4, 8, 84, 128, 128], P('gy', 'gx'), may hold values from -0.125 to 0.125
- gate_coords: int32 [4, 8, 84, 2], P('gy', 'gx'), may hold values from 0 to 13, as said below
- gate_count: int32 [4, 8], P('gy', 'gx'), may hold values from 28 to 84, as said below
- down_blocks: bfloat16 [8, 4, 48, 128, 128], P('gx', 'gy'), may hold values from -0.09375 to 0.09375
- down_rows: int32 [8, 4, 8], P('gx'), may hold values from 0 to 13, as said below
- down_coords: int32 [8, 4, 48, 2], P('gx', 'gy'), may hold values from 0 to 7, as said below
- down_count: int32 [8, 4], P('gx', 'gy'), may hold values from 16 to 48, as said below
Outputs:
- mixed: bfloat16 [512, 4096], P('gx', 'gy')
The draws below stay inside these ranges and needn't reach their ends.
Inputs may be any that keep to these rules, and one draw needn't show every extreme that they name: `gate_coords`: within each tile the 84 (model-width block, hidden block) pairs are distinct, the first below 8, the second below 14; only the first gate_count slots are live. `gate_count`: some tile has all 84 slots live. `down_rows`: within each down tile the 8 hidden blocks are distinct. `down_coords`: within each down tile the 48 (kept-row index below 8, model-width block below 8) pairs are distinct; only the first down_count slots are live. `down_count`: some tile has all 48 slots live.
All inputs are finite; a program needn't handle non-finite values.
Results may differ from the reference program's by a relative error of at most 0.025.
Values may be sent and summed in bfloat16 or wider, within the bound.
A program may use at most 64 MiB of HBM per device.

```python
import jax
import jax.numpy as jnp
from jax import lax

D = 4096
FF = 14336
BLOCK = 128
TOKENS = 512
DB = 8
FB = 14
CAP = 84
LOW = 28
USED = 8
CAPD = 48
LOWD = 16
N_GX = 8
N_GY = 4


def tile_pairs(key, tiles, positions, slots, inner):
    tile_keys = jax.random.split(key, tiles)
    orders = jax.vmap(lambda one_key: jax.random.permutation(one_key, positions))(tile_keys)[:, :slots]
    return jnp.stack([orders // inner, orders % inner], -1).astype(jnp.int32)


def tile_counts(key, tiles, lowest, highest):
    counts = jax.random.randint(key, (tiles,), lowest, highest + 1)
    chosen = jax.random.randint(jax.random.fold_in(key, 7), (), 0, tiles)
    return jnp.where(jnp.arange(tiles) == chosen, highest, counts).astype(jnp.int32)


def draw_gate_coords(key, part):
    pairs = tile_pairs(jax.random.fold_in(key, 11), N_GY * N_GX, DB * FB, CAP, FB)
    return pairs.reshape(N_GY, N_GX, CAP, 2)


def draw_gate_count(key, part):
    return tile_counts(jax.random.fold_in(key, 12), N_GY * N_GX, LOW, CAP).reshape(N_GY, N_GX)


def draw_down_rows(key, part):
    tile_keys = jax.random.split(jax.random.fold_in(key, 13), N_GX * N_GY)
    orders = jax.vmap(lambda one_key: jax.random.permutation(one_key, FB))(tile_keys)[:, :USED]
    return orders.astype(jnp.int32).reshape(N_GX, N_GY, USED)


def draw_down_coords(key, part):
    pairs = tile_pairs(jax.random.fold_in(key, 14), N_GX * N_GY, USED * DB, CAPD, DB)
    return pairs.reshape(N_GX, N_GY, CAPD, 2)


def draw_down_count(key, part):
    return tile_counts(jax.random.fold_in(key, 15), N_GX * N_GY, LOWD, CAPD).reshape(N_GX, N_GY)


def shard_levels(rng, shape, cuts, least, high):
    gain, own = 1.0, jax.random.fold_in(rng, 6)
    for dim, shards_of in cuts:
        steps = jnp.exp(jax.random.uniform(jax.random.fold_in(own, dim), (shards_of,), jnp.float32, least / len(cuts), high / len(cuts)))
        gain = gain * jnp.repeat(steps, shape[dim] // shards_of).reshape([-1 if axis == dim else 1 for axis in range(len(shape))])
    return gain


def centred(own_key, extent, scale, limit, cuts=(), held_as=jnp.bfloat16):
    gain = shard_levels(own_key, extent, cuts, -0.22, 0.18) if cuts else 1.0
    values = jax.random.normal(own_key, extent, jnp.float32) * scale * gain
    return jnp.minimum(jnp.maximum(values, -limit), limit).astype(held_as)


def setup_inputs(seed: int = 0) -> dict:
    arg_keys = jax.random.split(jax.random.key(seed), 10)
    tokens = centred(arg_keys[0], (TOKENS, D), 1.0, 6.0, ((0, 8), (1, 4)))
    gate_blocks = centred(arg_keys[1], (N_GY, N_GX, CAP, BLOCK, BLOCK), (D // 2) ** -0.5, 0.125, ((0, 4), (1, 8)))
    up_blocks = centred(arg_keys[2], (N_GY, N_GX, CAP, BLOCK, BLOCK), (D // 2) ** -0.5, 0.125, ((0, 4), (1, 8)))
    gate_coords = draw_gate_coords(jax.random.fold_in(arg_keys[9], 71), 0)
    gate_count = draw_gate_count(jax.random.fold_in(arg_keys[9], 71), 0)
    down_blocks = centred(arg_keys[5], (N_GX, N_GY, CAPD, BLOCK, BLOCK), (FF * 2 // 7) ** -0.5, 0.09375, ((0, 8), (1, 4)))
    down_rows = draw_down_rows(jax.random.fold_in(arg_keys[9], 71), 0)
    down_coords = draw_down_coords(jax.random.fold_in(arg_keys[9], 71), 0)
    down_count = draw_down_count(jax.random.fold_in(arg_keys[9], 71), 0)
    return dict(tokens=tokens, gate_blocks=gate_blocks, up_blocks=up_blocks, gate_coords=gate_coords, gate_count=gate_count, down_blocks=down_blocks, down_rows=down_rows, down_coords=down_coords, down_count=down_count)


def dense_matrix(blocks, local_rows, local_cols, counts, per_row, per_col, row_blocks, col_blocks):
    tiles_a, tiles_b, slots = blocks.shape[0], blocks.shape[1], blocks.shape[2]
    live_slots = jnp.arange(slots, dtype=jnp.int32)[None, None, :] < counts[:, :, None]
    global_rows = jnp.arange(tiles_a, dtype=jnp.int32)[:, None, None] * per_row + local_rows
    global_cols = jnp.arange(tiles_b, dtype=jnp.int32)[None, :, None] * per_col + local_cols
    values = jnp.where(live_slots[..., None, None], blocks, jnp.zeros((), blocks.dtype))
    grid = jnp.zeros((row_blocks, col_blocks, BLOCK, BLOCK), blocks.dtype)
    grid = grid.at[global_rows, global_cols].add(values)
    return grid.transpose(0, 2, 1, 3).reshape(row_blocks * BLOCK, col_blocks * BLOCK)


def rounded_sum(total, term):
    held = lax.optimization_barrier(term.astype(jnp.bfloat16))
    return total + held.astype(jnp.float32)


def reference(tokens, gate_blocks, up_blocks, gate_coords, gate_count, down_blocks, down_rows, down_coords, down_count):
    model_blocks = D // BLOCK
    hidden_blocks = FF // BLOCK
    gate_weight = dense_matrix(gate_blocks, gate_coords[..., 0], gate_coords[..., 1], gate_count, DB, FB, model_blocks, hidden_blocks)
    up_weight = dense_matrix(up_blocks, gate_coords[..., 0], gate_coords[..., 1], gate_count, DB, FB, model_blocks, hidden_blocks)
    kept_rows = jnp.take_along_axis(down_rows, down_coords[..., 0], axis=2)
    down_weight = dense_matrix(down_blocks, kept_rows, down_coords[..., 1], down_count, FB, DB, hidden_blocks, model_blocks)
    gate_total = jnp.zeros((TOKENS, FF), jnp.float32)
    up_total = jnp.zeros((TOKENS, FF), jnp.float32)
    width = DB * BLOCK
    for tile_row in range(N_GY):
        columns = tokens[:, tile_row * width:(tile_row + 1) * width]
        gate_total = rounded_sum(gate_total, jnp.dot(columns, gate_weight[tile_row * width:(tile_row + 1) * width], preferred_element_type=jnp.float32))
        up_total = rounded_sum(up_total, jnp.dot(columns, up_weight[tile_row * width:(tile_row + 1) * width], preferred_element_type=jnp.float32))
    hidden = (jax.nn.silu(gate_total) * up_total).astype(jnp.bfloat16)
    out_total = jnp.zeros((TOKENS, D), jnp.float32)
    span = FB * BLOCK
    for tile_col in range(N_GX):
        part_hidden = hidden[:, tile_col * span:(tile_col + 1) * span]
        out_total = rounded_sum(out_total, jnp.dot(part_hidden, down_weight[tile_col * span:(tile_col + 1) * span], preferred_element_type=jnp.float32))
    return out_total.astype(jnp.bfloat16)
```

```python
import functools

import jax
import jax.numpy as jnp
from jax import lax
from jax.experimental import pallas as pl
from jax.experimental.pallas import tpu as pltpu
from jax.sharding import PartitionSpec as P

BLOCK = 128
FF = 14336
MESH = pl.DeviceIdType.MESH
F32, BF16 = jnp.float32, jnp.bfloat16


def factor(n):
    low = 1
    while low * low * 4 <= n and n % (low * 2) == 0:
        low *= 2
    return n // low, low


def kernel(cfg, tab, tok, gblk, ublk, dblk, out, gw, uw, dw, wd, dd, gat, pa, pb,
           r1a, r1b, s2a, s2b, r2a, r2b, acca, accb, hid, a2s, a2r, ps, fr, facc,
           lsem, gs, gr, s1as, s1ar, s1bs, s1br, s2as, s2ar, s2bs, s2br, xs, xr, fs, fq):
    n_gx, n_gy, n_hi, n_lo, per, nc, rp, rows, n_model, fb, ca, cap, used, capd = cfg
    gx, gy = lax.axis_index("gx"), lax.axis_index("gy")
    zc, mc = gx // per, gx % per
    hi, lo = gy // n_lo, gy % n_lo
    loads = [
        pltpu.make_async_copy(gblk, gw.at[pl.ds(0, cap)], lsem.at[0]),
        pltpu.make_async_copy(ublk, uw.at[pl.ds(0, cap)], lsem.at[1]),
        pltpu.make_async_copy(dblk, dw.at[pl.ds(0, capd)], lsem.at[2]),
    ]
    for load in loads:
        load.start()
    barrier = pltpu.get_barrier_semaphore()
    for d in range(1, n_gy):
        pl.semaphore_signal(barrier, inc=1, device_id=(gx, (gy + d) % n_gy), device_id_type=MESH)
    for d in range(1, n_gx):
        pl.semaphore_signal(barrier, inc=1, device_id=((gx + d) % n_gx, gy), device_id_type=MESH)
    pl.semaphore_wait(barrier, n_gy + n_gx - 2)

    sends = []

    def send(src, dst, ssem, rsem, dev):
        copy = pltpu.make_async_remote_copy(
            src_ref=src, dst_ref=dst, send_sem=ssem, recv_sem=rsem,
            device_id=dev, device_id_type=MESH)
        copy.start()
        sends.append(copy)

    def arrived(ref, sem):
        pltpu.make_async_remote_copy(
            src_ref=ref, dst_ref=ref, send_sem=sem, recv_sem=sem,
            device_id=((gx + 1) % n_gx, gy), device_id_type=MESH).wait_recv()

    for o in range(nc):
        for j in range(per):
            if o == 0 and j == 0:
                continue
            cj = (mc + j) % per
            send(tok, gat.at[o, mc], gs.at[o, j], gr.at[o, mc], ((zc ^ o) * per + cj, gy))
    gat[0, mc] = tok[...]

    gw[cap] = jnp.zeros((BLOCK, BLOCK), BF16)
    uw[cap] = jnp.zeros((BLOCK, BLOCK), BF16)
    dw[capd] = jnp.zeros((BLOCK, BLOCK), BF16)
    loads[0].wait()
    loads[1].wait()

    def dense_col(c, _):
        at = pl.multiple_of(c * 2 * BLOCK, 2 * BLOCK)
        for r in range(n_model):
            slot = tab[r * fb + c]
            wd[pl.ds(r * BLOCK, BLOCK), pl.ds(at, BLOCK)] = gw[slot]
            wd[pl.ds(r * BLOCK, BLOCK), pl.ds(at + BLOCK, BLOCK)] = uw[slot]
        return 0

    lax.fori_loop(0, fb, dense_col, 0)
    down_at, rows_at = n_model * fb, n_model * fb + used * n_model

    def dense_down():
        loads[2].wait()

        def one(c, _):
            at = pl.multiple_of(c * BLOCK, BLOCK)
            for r in range(used):
                slot = tab[down_at + r * n_model + c]
                dd[pl.ds(r * BLOCK, BLOCK), pl.ds(at, BLOCK)] = dw[slot]
            return 0

        lax.fori_loop(0, n_model, one, 0)

    tall = per * rows

    def project(k):
        for j in range(per):
            if k == 0 and j == 0:
                continue
            c = (mc + j) % per
            arrived(gat.at[k, c], gr.at[k, c])
        for part, first, many in ((pa, 0, ca), (pb, ca, fb - ca)):
            def col(c, _, part=part, first=first):
                to = pl.multiple_of(c * 2 * BLOCK, 2 * BLOCK)
                at = pl.multiple_of((c + first) * 2 * BLOCK, 2 * BLOCK)
                y = jnp.dot(gat[k].reshape(tall, n_model * BLOCK),
                            wd[:, pl.ds(at, 2 * BLOCK)], preferred_element_type=F32)
                part[k, :, :, :, pl.ds(to, 2 * BLOCK)] = y.astype(BF16).reshape(
                    n_hi, n_lo, rp, 2 * BLOCK)
                return 0

            lax.fori_loop(0, many, col, 0)
            if part is pa:
                for d in range(1, n_lo):
                    l2 = (lo + d) % n_lo
                    send(pa.at[k, :, l2], r1a.at[k, d - 1], s1as.at[k, d - 1],
                         s1ar.at[k, d - 1], (gx, hi * n_lo + l2))
            else:
                for d in range(1, n_hi):
                    h2 = (hi + d) % n_hi
                    send(pb.at[k, h2], r1b.at[k, d - 1], s1bs.at[k, d - 1],
                         s1br.at[k, d - 1], (gx, h2 * n_lo + lo))

    def reduce_first(k):
        for d in range(1, n_lo):
            arrived(r1a.at[k, d - 1], s1ar.at[k, d - 1])
        for e in list(range(1, n_hi)) + [0]:
            h2 = (hi + e) % n_hi
            s = pa[k, h2, lo].astype(F32)
            for d in range(1, n_lo):
                s = s + r1a[k, d - 1, h2].astype(F32)
            if e == 0:
                acca[k] = s
            else:
                s2a[k, e - 1] = s.astype(BF16)
                send(s2a.at[k, e - 1], r2a.at[k, e - 1], s2as.at[k, e - 1],
                     s2ar.at[k, e - 1], (gx, h2 * n_lo + lo))
        for d in range(1, n_hi):
            arrived(r1b.at[k, d - 1], s1br.at[k, d - 1])
        for e in list(range(1, n_lo)) + [0]:
            l2 = (lo + e) % n_lo
            s = pb[k, hi, l2].astype(F32)
            for d in range(1, n_hi):
                s = s + r1b[k, d - 1, l2].astype(F32)
            if e == 0:
                accb[k] = s
            else:
                s2b[k, e - 1] = s.astype(BF16)
                send(s2b.at[k, e - 1], r2b.at[k, e - 1], s2bs.at[k, e - 1],
                     s2br.at[k, e - 1], (gx, hi * n_lo + l2))

    def activate(k):
        for d in range(1, n_hi):
            arrived(r2a.at[k, d - 1], s2ar.at[k, d - 1])
        for d in range(1, n_lo):
            arrived(r2b.at[k, d - 1], s2br.at[k, d - 1])
        for c in range(fb):
            acc, got, peers, at = (
                (acca, r2a, n_hi, c) if c < ca else (accb, r2b, n_lo, c - ca))
            cols = pl.ds(at * 2 * BLOCK, 2 * BLOCK)
            s = acc[k, :, cols]
            for d in range(1, peers):
                s = s + got[k, d - 1, :, cols].astype(F32)
            gate, up = s[:, :BLOCK], s[:, BLOCK:]
            hid[c] = (gate / (1.0 + jnp.exp(-gate)) * up).astype(BF16)
        for d in list(range(1, n_gy)) + [0]:
            dest = (gy + d) % n_gy
            for q in range(used):
                row = tab[rows_at + dest * used + q]
                cols = pl.ds(q * BLOCK, BLOCK)
                if d == 0:
                    a2r[k, 0, :, cols] = hid[row]
                else:
                    a2s[k, d - 1, :, cols] = hid[row]
            if d:
                send(a2s.at[k, d - 1], a2r.at[k, d], xs.at[k, d - 1],
                     xr.at[k, d - 1], (gx, dest))

    wide = 2 * BLOCK

    def mix(k):
        for d in range(1, n_gy):
            arrived(a2r.at[k, d], xr.at[k, d - 1])

        def col(c, _):
            at = pl.multiple_of(c * wide, wide)
            y = jnp.dot(a2r[k].reshape(n_gy * rp, used * BLOCK), dd[:, pl.ds(at, wide)],
                        preferred_element_type=F32).astype(BF16)
            for d in range(n_gy):
                own = (gy + n_gy - d) % n_gy
                ps[k, pl.ds(pl.multiple_of(own * rp, rp), rp), pl.ds(at, wide)] = (
                    y[d * rp:(d + 1) * rp])
            return 0

        lax.fori_loop(0, n_model * BLOCK // wide, col, 0)
        for j in range(per):
            if k == 0 and j == 0:
                continue
            cj = (mc + j) % per
            send(ps.at[k, pl.ds(pl.multiple_of(cj * rows, rows), rows)], fr.at[k, mc],
                 fs.at[k, j], fq.at[k, mc], ((zc ^ k) * per + cj, gy))
        if k == 0:
            facc[...] = ps[0, pl.ds(pl.multiple_of(mc * rows, rows), rows)].astype(F32)

    for s in range(nc + 3):
        if s < nc:
            project(s)
        if s == 1 or (nc == 1 and s == 0):
            dense_down()
        if 0 <= s - 1 < nc:
            reduce_first(s - 1)
        if 0 <= s - 2 < nc:
            activate(s - 2)
        if 0 <= s - 3 < nc:
            mix(s - 3)

    for k in range(nc):
        for j in range(per):
            if k == 0 and j == 0:
                continue
            c = (mc + j) % per
            arrived(fr.at[k, c], fq.at[k, c])
            facc[...] += fr[k, c].astype(F32)
    out[...] = facc[...].astype(BF16)
    for copy in sends:
        copy.wait_send()


def inverse(coords, count, row_count, col_count):
    slots = coords.shape[0]
    slot = jnp.arange(slots, dtype=jnp.int32)
    place = coords[:, 0] * col_count + coords[:, 1]
    spot = jnp.arange(row_count * col_count, dtype=jnp.int32)
    hit = (place[:, None] == spot[None, :]) & (slot < count)[:, None]
    return jnp.min(jnp.where(hit, slot[:, None], slots), axis=0)


def solution(mesh):
    n_gx, n_gy = mesh.shape["gx"], mesh.shape["gy"]
    n_hi, n_lo = factor(n_gy)
    per = 2 if n_gx % 2 == 0 else 1
    nc = n_gx // per

    def body(tokens, gate_blocks, up_blocks, gate_coords, gate_count,
             down_blocks, down_rows, down_coords, down_count):
        rows, width = tokens.shape
        n_model = width // BLOCK
        fb = FF // (BLOCK * n_gx)
        ca = (fb + 1) // 2
        cb = fb - ca
        cap, capd, used = gate_blocks.shape[2], down_blocks.shape[2], down_rows.shape[-1]
        rp = per * rows // n_gy
        tab = jnp.concatenate([
            inverse(gate_coords[0, 0], gate_count[0, 0], n_model, fb),
            inverse(down_coords[0, 0], down_count[0, 0], used, n_model),
            down_rows.reshape(-1),
        ])
        cfg = (n_gx, n_gy, n_hi, n_lo, per, nc, rp, rows, n_model, fb, ca, cap, used, capd)
        wa, wb = ca * 2 * BLOCK, cb * 2 * BLOCK
        kl, kh, kg = max(n_lo - 1, 1), max(n_hi - 1, 1), max(n_gy - 1, 1)
        vm, dma = pltpu.VMEM, pltpu.SemaphoreType.DMA
        hbm = pl.BlockSpec(memory_space=pltpu.HBM)
        return pl.pallas_call(
            functools.partial(kernel, cfg),
            out_shape=jax.ShapeDtypeStruct((rows, width), BF16),
            in_specs=[
                pl.BlockSpec(memory_space=pltpu.SMEM),
                pl.BlockSpec(memory_space=pltpu.VMEM),
                hbm, hbm, hbm,
            ],
            out_specs=pl.BlockSpec(memory_space=pltpu.VMEM),
            scratch_shapes=[
                vm((cap + 1, BLOCK, BLOCK), BF16),
                vm((cap + 1, BLOCK, BLOCK), BF16),
                vm((capd + 1, BLOCK, BLOCK), BF16),
                vm((width, fb * 2 * BLOCK), BF16),
                vm((used * BLOCK, width), BF16),
                vm((nc, per, rows, width), BF16),
                vm((nc, n_hi, n_lo, rp, wa), BF16),
                vm((nc, n_hi, n_lo, rp, wb), BF16),
                vm((nc, kl, n_hi, rp, wa), BF16),
                vm((nc, kh, n_lo, rp, wb), BF16),
                vm((nc, kh, rp, wa), BF16),
                vm((nc, kl, rp, wb), BF16),
                vm((nc, kh, rp, wa), BF16),
                vm((nc, kl, rp, wb), BF16),
                vm((nc, rp, wa), F32),
                vm((nc, rp, wb), F32),
                vm((fb, rp, BLOCK), BF16),
                vm((nc, kg, rp, used * BLOCK), BF16),
                vm((nc, n_gy, rp, used * BLOCK), BF16),
                vm((nc, per * rows, width), BF16),
                vm((nc, per, rows, width), BF16),
                vm((rows, width), F32),
                dma((3,)),
                dma((nc, per)), dma((nc, per)),
                dma((nc, kl)), dma((nc, kl)),
                dma((nc, kh)), dma((nc, kh)),
                dma((nc, kh)), dma((nc, kh)),
                dma((nc, kl)), dma((nc, kl)),
                dma((nc, kg)), dma((nc, kg)),
                dma((nc, per)), dma((nc, per)),
            ],
            compiler_params=pltpu.CompilerParams(
                collective_id=0, has_side_effects=True, vmem_limit_bytes=60 * 1024 * 1024),
        )(tab, tokens, gate_blocks.reshape(cap, BLOCK, BLOCK),
          up_blocks.reshape(cap, BLOCK, BLOCK), down_blocks.reshape(capd, BLOCK, BLOCK))

    return jax.shard_map(
        body,
        mesh=mesh,
        in_specs=(
            P("gx", "gy"),
            P("gy", "gx", None, None, None),
            P("gy", "gx", None, None, None),
            P("gy", "gx", None, None),
            P("gy", "gx"),
            P("gx", "gy", None, None, None),
            P("gx", None, None),
            P("gx", "gy", None, None),
            P("gx", "gy"),
        ),
        out_specs=P("gx", "gy"),
        check_vma=False,
    )
```

```python
import functools

import jax
import jax.numpy as jnp
from jax import lax
from jax.experimental import pallas as pl
from jax.experimental.pallas import tpu as pltpu
from jax.sharding import PartitionSpec as P

BLOCK = 128
FF = 14336
MESH = pl.DeviceIdType.MESH
F32, BF16 = jnp.float32, jnp.bfloat16


def factor(n):
    low = 1
    while low * low * 4 <= n and n % (low * 2) == 0:
        low *= 2
    return n // low, low


def kernel(cfg, tab, downs, kept, tok, gblk, ublk, dblk, out, gw, uw, dw, gat, pa, pb,
           r1a, r1b, s2a, s2b, r2a, r2b, acca, accb, hid, a2s, a2r, ps, fp, f2, fr, facc,
           lsem, gs, gr, s1as, s1ar, s1bs, s1br, s2as, s2ar, s2bs, s2br, xs, xr, fs, fq, fps, fpr):
    n_gx, n_gy, n_hi, n_lo, per, nc, rp, rows, n_model, fb, ca, cap, used, capd = cfg
    gx, gy = lax.axis_index("gx"), lax.axis_index("gy")
    zc, mc = gx // per, gx % per
    hi, lo = gy // n_lo, gy % n_lo
    loads = [
        pltpu.make_async_copy(gblk, gw.at[pl.ds(0, cap)], lsem.at[0]),
        pltpu.make_async_copy(ublk, uw.at[pl.ds(0, cap)], lsem.at[1]),
        pltpu.make_async_copy(dblk, dw.at[pl.ds(0, capd)], lsem.at[2]),
    ]
    for load in loads:
        load.start()
    barrier = pltpu.get_barrier_semaphore()
    for d in range(1, n_gy):
        pl.semaphore_signal(barrier, inc=1, device_id=(gx, (gy + d) % n_gy), device_id_type=MESH)
    for d in range(1, n_gx):
        pl.semaphore_signal(barrier, inc=1, device_id=((gx + d) % n_gx, gy), device_id_type=MESH)
    pl.semaphore_wait(barrier, n_gy + n_gx - 2)

    sends = []

    def send(src, dst, ssem, rsem, dev):
        copy = pltpu.make_async_remote_copy(
            src_ref=src, dst_ref=dst, send_sem=ssem, recv_sem=rsem,
            device_id=dev, device_id_type=MESH)
        copy.start()
        sends.append(copy)

    def arrived(ref, sem):
        pltpu.make_async_remote_copy(
            src_ref=ref, dst_ref=ref, send_sem=sem, recv_sem=sem,
            device_id=((gx + 1) % n_gx, gy), device_id_type=MESH).wait_recv()

    order = list(range(nc))
    for j in range(1, per):
        send(tok, gat.at[0, mc], gs.at[0, j], gr.at[0, mc], (zc * per + (mc + j) % per, gy))
    for o in order:
        if o:
            send(tok, gat.at[o, mc], gs.at[o, 0], gr.at[o, mc], ((zc ^ o) * per + mc, gy))
    gat[0, mc] = tok[...]

    def relay(o):
        if o:
            arrived(gat.at[o, mc], gr.at[o, mc])
            for j in range(1, per):
                send(gat.at[o, mc], gat.at[o, mc], gs.at[o, j], gr.at[o, mc],
                     (zc * per + (mc + j) % per, gy))

    gw[cap] = jnp.zeros((BLOCK, BLOCK), BF16)
    uw[cap] = jnp.zeros((BLOCK, BLOCK), BF16)
    dw[capd] = jnp.zeros((BLOCK, BLOCK), BF16)
    loads[0].wait()
    loads[1].wait()

    tall = per * rows

    def project(k):
        for j in range(1, per):
            c = (mc + j) % per
            arrived(gat.at[k, c], gr.at[k, c])
        for part, first, many in ((pa, 0, ca), (pb, ca, fb - ca)):
            def col(c, _, part=part, first=first):
                to = pl.multiple_of(c * 2 * BLOCK, 2 * BLOCK)
                slots = [tab[r * fb + c + first] for r in range(n_model)]
                weight = jnp.concatenate(
                    [jnp.concatenate([gw[i], uw[i]], axis=1) for i in slots], axis=0)
                y = jnp.dot(gat[k].reshape(tall, n_model * BLOCK), weight,
                            preferred_element_type=F32)
                part[k, :, :, :, pl.ds(to, 2 * BLOCK)] = y.astype(BF16).reshape(
                    n_hi, n_lo, rp, 2 * BLOCK)
                return 0

            lax.fori_loop(0, many, col, 0, unroll=True)
            if part is pa:
                for d in range(1, n_lo):
                    l2 = (lo + d) % n_lo
                    send(pa.at[k, :, l2], r1a.at[k, d - 1], s1as.at[k, d - 1],
                         s1ar.at[k, d - 1], (gx, hi * n_lo + l2))
            else:
                for d in range(1, n_hi):
                    h2 = (hi + d) % n_hi
                    send(pb.at[k, h2], r1b.at[k, d - 1], s1bs.at[k, d - 1],
                         s1br.at[k, d - 1], (gx, h2 * n_lo + lo))

    def reduce_first(k):
        for d in range(1, n_lo):
            arrived(r1a.at[k, d - 1], s1ar.at[k, d - 1])
        for e in list(range(1, n_hi)) + [0]:
            h2 = (hi + e) % n_hi
            s = pa[k, h2, lo].astype(F32)
            for d in range(1, n_lo):
                s = s + r1a[k, d - 1, h2].astype(F32)
            if e == 0:
                acca[k] = s
            else:
                s2a[k, e - 1] = s.astype(BF16)
                send(s2a.at[k, e - 1], r2a.at[k, e - 1], s2as.at[k, e - 1],
                     s2ar.at[k, e - 1], (gx, h2 * n_lo + lo))
        for d in range(1, n_hi):
            arrived(r1b.at[k, d - 1], s1br.at[k, d - 1])
        for e in list(range(1, n_lo)) + [0]:
            l2 = (lo + e) % n_lo
            s = pb[k, hi, l2].astype(F32)
            for d in range(1, n_hi):
                s = s + r1b[k, d - 1, l2].astype(F32)
            if e == 0:
                accb[k] = s
            else:
                s2b[k, e - 1] = s.astype(BF16)
                send(s2b.at[k, e - 1], r2b.at[k, e - 1], s2bs.at[k, e - 1],
                     s2br.at[k, e - 1], (gx, hi * n_lo + l2))

    def activate(k):
        for d in range(1, n_hi):
            arrived(r2a.at[k, d - 1], s2ar.at[k, d - 1])
        for d in range(1, n_lo):
            arrived(r2b.at[k, d - 1], s2br.at[k, d - 1])
        for c in range(fb):
            acc, got, peers, at = (
                (acca, r2a, n_hi, c) if c < ca else (accb, r2b, n_lo, c - ca))
            cols = pl.ds(at * 2 * BLOCK, 2 * BLOCK)
            s = acc[k, :, cols]
            for d in range(1, peers):
                s = s + got[k, d - 1, :, cols].astype(F32)
            gate, up = s[:, :BLOCK], s[:, BLOCK:]
            hid[c] = (gate / (1.0 + jnp.exp(-gate)) * up).astype(BF16)
        for d in list(range(1, n_gy)) + [0]:
            dest = (gy + d) % n_gy
            for q in range(used):
                row = kept[0, dest, q]
                cols = pl.ds(q * BLOCK, BLOCK)
                if d == 0:
                    a2r[k, 0, :, cols] = hid[row]
                else:
                    a2s[k, d - 1, :, cols] = hid[row]
            if d:
                send(a2s.at[k, d - 1], a2r.at[k, d], xs.at[k, d - 1],
                     xr.at[k, d - 1], (gx, dest))

    wide = 2 * BLOCK

    def mix(k):
        for d in range(1, n_gy):
            arrived(a2r.at[k, d], xr.at[k, d - 1])

        def col(c, _):
            at = pl.multiple_of(c * wide, wide)
            slots = [[downs[r * n_model + c * 2 + i] for i in range(2)]
                     for r in range(used)]
            weight = jnp.concatenate(
                [jnp.concatenate([dw[i] for i in pair], axis=1) for pair in slots], axis=0)
            y = jnp.dot(a2r[k].reshape(n_gy * rp, used * BLOCK), weight,
                        preferred_element_type=F32).astype(BF16)
            for d in range(n_gy):
                own = (gy + n_gy - d) % n_gy
                ps[k, pl.ds(pl.multiple_of(own * rp, rp), rp), pl.ds(at, wide)] = (
                    y[d * rp:(d + 1) * rp])
            return 0

        lax.fori_loop(0, n_model * BLOCK // wide, col, 0)
        for j in range(1, per):
            cj = (mc + j) % per
            send(ps.at[k, pl.ds(pl.multiple_of(cj * rows, rows), rows)], fp.at[k, j - 1],
                 fps.at[k, j - 1], fpr.at[k, j - 1], (zc * per + cj, gy))

    def finish(k):
        s = ps[k, pl.ds(pl.multiple_of(mc * rows, rows), rows)].astype(F32)
        for j in range(1, per):
            arrived(fp.at[k, j - 1], fpr.at[k, j - 1])
            s = s + fp[k, j - 1].astype(F32)
        if k:
            f2[k] = s.astype(BF16)
            send(f2.at[k], fr.at[k], fs.at[k], fq.at[k], ((zc ^ k) * per + mc, gy))
        else:
            facc[...] = s

    relay(order[0])
    for s in range(nc + 4):
        if s < nc:
            project(order[s])
        if s + 1 < nc:
            relay(order[s + 1])
        if s == 0:
            loads[2].wait()
        if 0 <= s - 1 < nc:
            reduce_first(order[s - 1])
        if 0 <= s - 4 < nc:
            finish(order[s - 4])
        if 0 <= s - 2 < nc:
            activate(order[s - 2])
        if 0 <= s - 3 < nc:
            mix(order[s - 3])

    for k in order:
        if k:
            arrived(fr.at[k], fq.at[k])
            facc[...] += fr[k].astype(F32)
    out[...] = facc[...].astype(BF16)
    for copy in sends:
        copy.wait_send()


def inverse(coords, count, row_count, col_count):
    slots = coords.shape[0]
    slot = jnp.arange(slots, dtype=jnp.int32)
    place = coords[:, 0] * col_count + coords[:, 1]
    spot = jnp.arange(row_count * col_count, dtype=jnp.int32)
    hit = (place[:, None] == spot[None, :]) & (slot < count)[:, None]
    return jnp.min(jnp.where(hit, slot[:, None], slots), axis=0)


def solution(mesh):
    n_gx, n_gy = mesh.shape["gx"], mesh.shape["gy"]
    n_hi, n_lo = factor(n_gy)
    per = 2 if n_gx % 2 == 0 else 1
    nc = n_gx // per

    def body(tokens, gate_blocks, up_blocks, gate_coords, gate_count,
             down_blocks, down_rows, down_coords, down_count):
        rows, width = tokens.shape
        n_model = width // BLOCK
        fb = FF // (BLOCK * n_gx)
        ca = (fb + 1) // 2
        cb = fb - ca
        cap, capd, used = gate_blocks.shape[2], down_blocks.shape[2], down_rows.shape[-1]
        rp = per * rows // n_gy
        tab = inverse(gate_coords[0, 0], gate_count[0, 0], n_model, fb)
        downs = inverse(down_coords[0, 0], down_count[0, 0], used, n_model)
        cfg = (n_gx, n_gy, n_hi, n_lo, per, nc, rp, rows, n_model, fb, ca, cap, used, capd)
        wa, wb = ca * 2 * BLOCK, cb * 2 * BLOCK
        kl, kh, kg = max(n_lo - 1, 1), max(n_hi - 1, 1), max(n_gy - 1, 1)
        vm, dma = pltpu.VMEM, pltpu.SemaphoreType.DMA
        hbm = pl.BlockSpec(memory_space=pltpu.HBM)
        return pl.pallas_call(
            functools.partial(kernel, cfg),
            out_shape=jax.ShapeDtypeStruct((rows, width), BF16),
            in_specs=[
                pl.BlockSpec(memory_space=pltpu.SMEM),
                pl.BlockSpec(memory_space=pltpu.SMEM),
                pl.BlockSpec(memory_space=pltpu.SMEM),
                pl.BlockSpec(memory_space=pltpu.VMEM),
                hbm, hbm, hbm,
            ],
            out_specs=pl.BlockSpec(memory_space=pltpu.VMEM),
            scratch_shapes=[
                vm((cap + 1, BLOCK, BLOCK), BF16),
                vm((cap + 1, BLOCK, BLOCK), BF16),
                vm((capd + 1, BLOCK, BLOCK), BF16),
                vm((nc, per, rows, width), BF16),
                vm((nc, n_hi, n_lo, rp, wa), BF16),
                vm((nc, n_hi, n_lo, rp, wb), BF16),
                vm((nc, kl, n_hi, rp, wa), BF16),
                vm((nc, kh, n_lo, rp, wb), BF16),
                vm((nc, kh, rp, wa), BF16),
                vm((nc, kl, rp, wb), BF16),
                vm((nc, kh, rp, wa), BF16),
                vm((nc, kl, rp, wb), BF16),
                vm((nc, rp, wa), F32),
                vm((nc, rp, wb), F32),
                vm((fb, rp, BLOCK), BF16),
                vm((nc, kg, rp, used * BLOCK), BF16),
                vm((nc, n_gy, rp, used * BLOCK), BF16),
                vm((nc, per * rows, width), BF16),
                vm((nc, max(per - 1, 1), rows, width), BF16),
                vm((nc, rows, width), BF16),
                vm((nc, rows, width), BF16),
                vm((rows, width), F32),
                dma((3,)),
                dma((nc, per)), dma((nc, per)),
                dma((nc, kl)), dma((nc, kl)),
                dma((nc, kh)), dma((nc, kh)),
                dma((nc, kh)), dma((nc, kh)),
                dma((nc, kl)), dma((nc, kl)),
                dma((nc, kg)), dma((nc, kg)),
                dma((nc,)), dma((nc,)),
                dma((nc, max(per - 1, 1))), dma((nc, max(per - 1, 1))),
            ],
            compiler_params=pltpu.CompilerParams(
                collective_id=0, has_side_effects=True, vmem_limit_bytes=60 * 1024 * 1024),
        )(tab, downs, down_rows, tokens, gate_blocks.reshape(cap, BLOCK, BLOCK),
          up_blocks.reshape(cap, BLOCK, BLOCK), down_blocks.reshape(capd, BLOCK, BLOCK))

    return jax.shard_map(
        body,
        mesh=mesh,
        in_specs=(
            P("gx", "gy"),
            P("gy", "gx", None, None, None),
            P("gy", "gx", None, None, None),
            P("gy", "gx", None, None),
            P("gy", "gx"),
            P("gx", "gy", None, None, None),
            P("gx", None, None),
            P("gx", "gy", None, None),
            P("gx", "gy"),
        ),
        out_specs=P("gx", "gy"),
        check_vma=False,
    )
```
